32 devices in a mesh: groups: 2 (over y), tile: 4 (over z), tracer: 4 (over x, core).
Axes of the slice: x: 2, y: 2, z: 4, core: 2. Of those that a mesh axis runs over, the one named last changes fastest.
Arguments:
- species_amounts: float32 [64, 32, 128, 128], P(('groups', 'tracer'), None, 'tile'), parts along dimension 0, may hold values from 0.2 to 2
- face_currents: float32 [2, 64, 128, 128], P(None, 'groups', 'tile'), parts along dimension 1, may hold values from -1 to 1
- thermal_anomaly: float32 [64, 128, 128], P(('groups', 'tracer'), 'tile'), parts along dimension 0, may hold values from -4 to 4
- layer_total_per_profile: int32 [256, 128], P(('groups', 'tile')), parts along dimension 0, may hold values from 0 to 32
- consumed_species: int32 [32], replicated, may hold values from 0 to 31, each once
- attenuation_factor: float32 [32], replicated, may hold values from 0.009375 to 0.09375
- intake_speedup: float32 [32], replicated, may hold values from 0.3 to 3
- incoming_sunshine: float32 [256, 128], P(('groups', 'tile')), parts along dimension 0, may hold values from 0.5 to 2
Outputs:
- tracers_out: float32 [64, 32, 128, 128], P('groups', 'tracer', 'tile'), parts along dimension 0
- velocity_out: float32 [2, 64, 128, 128], P(None, ('groups', 'tracer'), 'tile'), parts along dimension 1
- temperature_out: float32 [64, 128, 128], P(('groups', 'tracer'), 'tile'), parts along dimension 0
The draws below stay inside these ranges and needn't reach their ends.
There are 2 independent parts, one for each index of `groups`. The reference program is written for one: setup_inputs(seed, part) draws one part's arguments, and reference() takes and returns one part's arrays. A program takes and returns all parts, laid end to end along the dimension named above; an argument that names none is the same for every part. Nothing has to cross between parts.
Inputs may be any that keep to these rules, and one draw needn't show every extreme that they name: Levels 0 to layer_total_per_profile - 1 of a column are sea, deeper levels are land; 0 marks a land column. `consumed_species`: A permutation of the 32 tracers.
All inputs are finite; a program needn't handle non-finite values.
Results may differ from the reference program's by a relative error of at most 0.0003.
Values sent between devices are 32-bit elements; how exact they have to be, the bound alone decides.
A program may use at most 64 MiB of HBM per device.

```python
import math
import jax
import jax.numpy as jnp
from jax import lax

NTR = 32
DEPTH_LAYERS = 32
GRID_MERIDIONAL = 128
GRID_ZONAL = 128


def place_ends(entries, rng, smallest, largest):
    extent = entries.shape
    place = [jax.random.randint(jax.random.fold_in(rng, axis), (), 0, extent[axis]) for axis in range(len(extent))]
    entries = entries.at[tuple(place)].set(smallest)
    longest = extent.index(max(extent))
    place[longest] = (place[longest] + 1) % extent[longest]
    return entries.at[tuple(place)].set(largest)


def level_of(rng, shape, shards, least, largest):
    loudness = 1.0
    for axis_at, parts in shards:
        draws = jax.random.uniform(jax.random.fold_in(jax.random.fold_in(rng, 6), axis_at), (parts,), jnp.float32, least / len(shards), largest / len(shards))
        loudness = loudness * jnp.repeat(jnp.exp(draws), shape[axis_at] // parts).reshape((-1,) + (1,) * (len(shape) - 1 - axis_at))
    return loudness


def scatter_about(stream_key, dims, deviation, bound, pieces=(), held_as=jnp.bfloat16):
    loudness = level_of(stream_key, dims, pieces, -0.22, 0.18) if pieces else 1.0
    array = jax.random.normal(stream_key, dims, jnp.float32) * deviation * loudness
    return jnp.minimum(jnp.maximum(array, -bound), bound).astype(held_as)


def setup_inputs(seed: int = 0, part: int = 0) -> dict:
    key_list = jax.random.split(jax.random.key(seed), 9)
    part_splits = jax.random.split(jax.random.fold_in(key_list[8], part), 9)
    return {
        "species_amounts": jnp.clip(jnp.exp(math.log(2.0) - 2.3025851 * jax.random.uniform(part_splits[0], (NTR, DEPTH_LAYERS, GRID_ZONAL, GRID_MERIDIONAL), jnp.float32) ** level_of(part_splits[0], (NTR, DEPTH_LAYERS, GRID_ZONAL, GRID_MERIDIONAL), ((0, 4), (2, 4)), -0.2, 0.2)), 0.2, 2.0),
        "face_currents": jnp.clip(jax.random.uniform(part_splits[1], (2, DEPTH_LAYERS, GRID_ZONAL, GRID_MERIDIONAL), jnp.float32, -1.0, 1.0) * level_of(part_splits[1], (2, DEPTH_LAYERS, GRID_ZONAL, GRID_MERIDIONAL), ((2, 4),), -0.4, 0.0), -1.0, 1.0),
        "thermal_anomaly": scatter_about(part_splits[2], (DEPTH_LAYERS, GRID_ZONAL, GRID_MERIDIONAL), 1.0, 4.0, ((0, 4), (1, 4)), jnp.float32),
        "layer_total_per_profile": place_ends(jax.random.randint(part_splits[3], (GRID_ZONAL, GRID_MERIDIONAL), 0, DEPTH_LAYERS + 1), jax.random.fold_in(part_splits[3], 1), 0, DEPTH_LAYERS).astype(jnp.int32),
        "consumed_species": jax.random.permutation(key_list[4], NTR).astype(jnp.int32),
        "attenuation_factor": jnp.clip(jnp.exp(jax.random.uniform(key_list[5], (NTR,), jnp.float32, math.log(0.009375), math.log(0.09375))), 0.009375, 0.09375),
        "intake_speedup": jnp.clip(jnp.exp(jax.random.uniform(key_list[6], (NTR,), jnp.float32, math.log(0.3), math.log(3.0))), 0.3, 3.0),
        "incoming_sunshine": jnp.clip(jnp.exp(math.log(2.0) - 1.3862944 * jax.random.uniform(part_splits[7], (GRID_ZONAL, GRID_MERIDIONAL), jnp.float32) ** level_of(part_splits[7], (GRID_ZONAL, GRID_MERIDIONAL), ((0, 4),), -0.2, 0.2)), 0.5, 2.0),
    }


sub_step = 0.45
step_duration = 0.2
gravity = 0.5
viscosity = 0.2
coriolis_base = 0.5
beta_plane = 0.5
spreading_coefficient = 0.2
water_clear = 0.05
column_optical = 3.0
warming_coefficient = 5.0
light_half = 0.3
nutrient_half = 0.5


def wraparound_border(values, margin, along):
    length = values.shape[along]
    leading = lax.slice_in_dim(values, length - margin, length, axis=along)
    trailing = lax.slice_in_dim(values, 0, margin, axis=along)
    return jnp.concatenate([leading, values, trailing], axis=along)


def shift_south(values):
    return jnp.concatenate([jnp.zeros_like(values[..., :1]), values[..., :-1]], axis=-1)


def shift_north(values, offset=1):
    return jnp.concatenate([values[..., offset:], jnp.zeros_like(values[..., :offset])], axis=-1)


def wet_levels(depth_ext, first_level, level_count):
    levels = first_level + jnp.arange(level_count, dtype=jnp.int32)
    return (levels[:, None, None] < depth_ext[None]).astype(jnp.float32)


def limiter(left_slope, right_slope):
    smaller = jnp.minimum(jnp.abs(left_slope), jnp.abs(right_slope))
    return jnp.where(left_slope * right_slope > 0.0, jnp.sign(left_slope) * smaller, 0.0)


def face_flux(behind, centre, forward, beyond, speed):
    positive = speed * (centre + 0.5 * limiter(centre - behind, forward - centre))
    negative = speed * (forward - 0.5 * limiter(forward - centre, beyond - forward))
    return jnp.where(speed > 0.0, positive, negative)


def face_speeds(velocity_with_halo_border, wet_ext):
    east_speed = velocity_with_halo_border[0][:, :-1] * wet_ext[:, :-1] * wet_ext[:, 1:]
    north_speed = velocity_with_halo_border[1] * wet_ext * shift_north(wet_ext)
    return east_speed, north_speed


def flux_substep(extended, east_speed, north_speed):
    length = extended.shape[2]
    east_flux = face_flux(extended[:, :, 0:length - 3], extended[:, :, 1:length - 2],
                          extended[:, :, 2:length - 1], extended[:, :, 3:length],
                          east_speed[:, 1:length - 2])
    middle = extended[:, :, 2:length - 2]
    north_flux = face_flux(shift_south(middle), middle, shift_north(middle), shift_north(middle, 2),
                           north_speed[:, 2:length - 2])
    spread = (east_flux[:, :, 1:] - east_flux[:, :, :-1]) + (north_flux - shift_south(north_flux))
    return middle - sub_step * spread


def laplacian(values):
    inner = values[:, 1:-1]
    return values[:, 2:] + values[:, :-2] + shift_north(inner) + shift_south(inner) - 4.0 * inner


def velocity_advance(flow_one, marine_mask_profile, thermal_profile_alone):
    east_vel = flow_one[0]
    north_vel = flow_one[1]
    ocean_profiles = east_vel.shape[1] - 2
    coriolis_y = coriolis_base + beta_plane * jnp.arange(east_vel.shape[2], dtype=jnp.float32) / east_vel.shape[2]
    centre_u = east_vel[:, 1:ocean_profiles + 1]
    centre_v = north_vel[:, 1:ocean_profiles + 1]
    v_bar = 0.25 * (centre_v + north_vel[:, 2:] + shift_south(centre_v) + shift_south(north_vel[:, 2:]))
    u_bar = 0.25 * (centre_u + east_vel[:, :-2] + shift_north(centre_u) + shift_north(east_vel[:, :-2]))
    marine_mask_interior = marine_mask_profile[:, 1:ocean_profiles + 1]
    east_open = marine_mask_interior * marine_mask_profile[:, 2:]
    north_open = marine_mask_interior * shift_north(marine_mask_interior)
    heat_mid = thermal_profile_alone[:, 1:ocean_profiles + 1]
    new_east = east_open * (centre_u + step_duration * (coriolis_y * v_bar - gravity * (thermal_profile_alone[:, 2:] - heat_mid)
                                                    + viscosity * laplacian(east_vel)))
    new_north = north_open * (centre_v + step_duration * (-coriolis_y * u_bar - gravity * (shift_north(heat_mid) - heat_mid)
                                                      + viscosity * laplacian(north_vel)))
    return jnp.stack([new_east, new_north]), laplacian(thermal_profile_alone)


def optical_thickness(by_cells, attenuation_factor):
    summed = jnp.tensordot(attenuation_factor, jnp.abs(by_cells), axes=1, precision=lax.Precision.HIGHEST)
    return (water_clear + summed) * (column_optical / DEPTH_LAYERS)


def react(by_cells, optical, overhead, wet_mask, incoming_sunshine, intake_speedup, consumed_species):
    depth_tau = overhead[None] + (jnp.cumsum(optical, axis=0) - optical)
    reaching = incoming_sunshine[None] * jnp.exp(-depth_tau)
    absorbed_part = 1.0 - jnp.exp(-optical)
    captured_radiance = reaching * absorbed_part * wet_mask
    mean_light = reaching * absorbed_part / optical
    light_limit = mean_light / (mean_light + light_half)
    pairing = (consumed_species[:, None] == jnp.arange(by_cells.shape[0], dtype=jnp.int32)[None]).astype(jnp.float32)
    nutrient = jnp.tensordot(pairing, by_cells, axes=1, precision=lax.Precision.HIGHEST)
    uptake = intake_speedup[:, None, None, None] * light_limit[None] * by_cells * nutrient / (nutrient_half + jnp.abs(nutrient))
    consumed = jnp.tensordot(pairing.T, uptake, axes=1, precision=lax.Precision.HIGHEST)
    updated = by_cells + wet_mask[None] * (uptake - consumed)
    return updated, captured_radiance


def reference(species_amounts, face_currents, thermal_anomaly, layer_total_per_profile, consumed_species, attenuation_factor, intake_speedup, incoming_sunshine):
    wet_ext = wet_levels(wraparound_border(layer_total_per_profile, 2, 0), 0, DEPTH_LAYERS)
    velocity_with_halo_border = wraparound_border(face_currents, 2, 2)
    east_speed, north_speed = face_speeds(velocity_with_halo_border, wet_ext)

    def advect_one(single):
        values = single[None]
        for repeat in range(2):
            values = flux_substep(wraparound_border(values, 2, 2), east_speed, north_speed)
        return values[0]

    advected = lax.map(advect_one, species_amounts)
    marine_mask_profile = wet_ext[:, 1:-1]
    advanced_face_speeds, thermal_second_derivative = velocity_advance(velocity_with_halo_border[:, :, 1:-1], marine_mask_profile, wraparound_border(thermal_anomaly, 1, 1))
    marine_mask_interior = marine_mask_profile[:, 1:-1]
    optical = optical_thickness(advected, attenuation_factor)
    overhead = jnp.zeros(optical.shape[1:], jnp.float32)
    updated, captured_radiance = react(advected, optical, overhead, marine_mask_interior, incoming_sunshine, intake_speedup, consumed_species)
    advanced_thermal_field = marine_mask_interior * (thermal_anomaly + step_duration * spreading_coefficient * thermal_second_derivative + warming_coefficient * captured_radiance)
    return updated, advanced_face_speeds, advanced_thermal_field
```

```python
import functools

import jax
import jax.numpy as jnp
from jax import lax
from jax.experimental import pallas as pl
from jax.experimental.pallas import tpu as pltpu
from jax.sharding import PartitionSpec as P

MESH = pl.DeviceIdType.MESH

sub_step = 0.45
step_duration = 0.2
gravity = 0.5
viscosity = 0.2
coriolis_base = 0.5
beta_plane = 0.5
spreading_coefficient = 0.2
water_clear = 0.05
column_optical = 3.0
warming_coefficient = 5.0
light_half = 0.3
nutrient_half = 0.5

PAD = 8
EDGE = 4


def lane_index(shape):
    return lax.broadcasted_iota(jnp.int32, shape, len(shape) - 1)


def east(x):
    return pltpu.roll(x, x.shape[0] - 1, 0)


def west(x):
    return pltpu.roll(x, 1, 0)


def north(x):
    return jnp.where(lane_index(x.shape) == x.shape[1] - 1, 0.0, pltpu.roll(x, x.shape[1] - 1, 1))


def south(x):
    return jnp.where(lane_index(x.shape) == 0, 0.0, pltpu.roll(x, 1, 1))


def minmod(a, b):
    return jnp.maximum(jnp.minimum(a, b), 0.0) + jnp.minimum(jnp.maximum(a, b), 0.0)


def laplacian(x):
    return east(x) + west(x) + north(x) + south(x) - 4.0 * x


def substep(c, es, ns, lane):
    last = c.shape[1] - 1
    d = east(c) - c
    half = 0.5 * minmod(west(d), d)
    flux = es * jnp.where(es > 0.0, c + half, east(c - half))
    spread = flux - west(flux)
    d = jnp.where(lane == last, 0.0, pltpu.roll(c, last, 1)) - c
    half = 0.5 * minmod(jnp.where(lane == 0, c, pltpu.roll(d, 1, 1)), d)
    flux = ns * jnp.where(ns > 0.0, c + half, pltpu.roll(c - half, last, 1))
    return c - (spread + (flux - pltpu.roll(flux, 1, 1)))


def transport_kernel(
    tiles, ranks, cores, q,
    sp, fc, th, dep, att,
    cells, over, vel, heat,
    ext, fext, hext, dext, adv, tot, pre,
    h_send, h_recv, f_send, f_recv, s_send, s_recv, d_send, d_recv, o_send, o_recv,
    l_sem, lf_sem, ls_sem, own_sem,
):
    nt, nl, rows, width = sp.shape
    per = nl // ranks
    nc = per // q
    chips = ranks // cores
    chunks = ranks * nc
    full = rows + 2 * PAD
    r = lax.axis_index("tracer")
    z = lax.axis_index("tile")
    a, b = r // cores, lax.rem(r, cores)
    up, down = lax.rem(z + 1, tiles), lax.rem(z + tiles - 1, tiles)

    def target(s):
        ka, kb = lax.rem(1 + s // cores, chips), cores - 1 - lax.rem(s, cores)
        return lax.rem(a + ka, chips) * cores + lax.rem(b + kb, cores)

    def source(s):
        ka, kb = lax.rem(1 + s // cores, chips), cores - 1 - lax.rem(s, cores)
        return lax.rem(a + chips - ka, chips) * cores + lax.rem(b + cores - kb, cores)

    def first_level(n):
        return target(n // nc) * per + lax.rem(n, nc) * q

    low_rows = pl.ds(0, EDGE)
    high_rows = pl.ds(rows - EDGE, EDGE)
    from_low = pl.ds(PAD - EDGE, EDGE)
    from_high = pl.ds(PAD + rows, EDGE)
    body = pl.ds(PAD, rows)

    def pair(src, dst, lead, send, recv, at):
        return (
            pltpu.make_async_remote_copy(
                src.at[lead + (high_rows,)], dst.at[lead + (from_low,)],
                send.at[at + (0,)], recv.at[at + (0,)],
                device_id={"tile": up}, device_id_type=MESH,
            ),
            pltpu.make_async_remote_copy(
                src.at[lead + (low_rows,)], dst.at[lead + (from_high,)],
                send.at[at + (1,)], recv.at[at + (1,)],
                device_id={"tile": down}, device_id_type=MESH,
            ),
        )

    def species_edges(n):
        lead = (slice(None), pl.ds(first_level(n), q))
        return pair(sp, ext, lead, h_send, h_recv, (n,))

    def current_edges(n):
        lead = (slice(None), pl.ds(first_level(n), q))
        return pair(fc, fext, lead, f_send, f_recv, (n,))

    def heat_edges():
        return pair(th, hext, (slice(None),), s_send, s_recv, (0,))

    def depth_edges():
        return pair(dep, dext, (), s_send, s_recv, (1,))

    def species_local(n):
        lev = pl.ds(first_level(n), q)
        return pltpu.make_async_copy(sp.at[:, lev], ext.at[:, lev, body], l_sem.at[n])

    def block_copy(n):
        s, c = n // nc, lax.rem(n, nc)
        return pltpu.make_async_remote_copy(
            adv.at[:, pl.ds(first_level(n), q)],
            cells.at[pl.ds(r * nt, nt), pl.ds(c * q, q)],
            d_send.at[n], d_recv.at[n],
            device_id={"tracer": target(s)}, device_id_type=MESH,
        )

    def block_arrival(n):
        s, c = n // nc, lax.rem(n, nc)
        return pltpu.make_async_remote_copy(
            adv.at[:, pl.ds(first_level(n), q)],
            cells.at[pl.ds(source(s) * nt, nt), pl.ds(c * q, q)],
            d_send.at[n], d_recv.at[n],
            device_id={"tracer": target(s)}, device_id_type=MESH,
        )

    def own_copy(n):
        c = lax.rem(n, nc)
        return pltpu.make_async_copy(
            adv.at[:, pl.ds(first_level(n), q)],
            cells.at[pl.ds(r * nt, nt), pl.ds(c * q, q)],
            own_sem.at[c],
        )

    def over_copy(s, place):
        return pltpu.make_async_remote_copy(
            pre.at[target(s)], over.at[place], o_send.at[s], o_recv.at[s],
            device_id={"tracer": target(s)}, device_id_type=MESH,
        )

    fc_local = pltpu.make_async_copy(fc, fext.at[:, :, body], lf_sem.at[0])
    dep_local = pltpu.make_async_copy(dep, dext.at[body], lf_sem.at[1])
    th_local = pltpu.make_async_copy(th, hext.at[:, body], lf_sem.at[2])
    dep_local.start()
    fc_local.start()

    def start_local(n, carry):
        species_local(n).start()
        return carry

    lax.fori_loop(0, chunks, start_local, 0)
    th_local.start()

    barrier = pltpu.get_barrier_semaphore()
    for place in (up, down):
        pl.semaphore_signal(barrier, inc=1, device_id={"tile": place}, device_id_type=MESH)
    for s in range(ranks - 1):
        pl.semaphore_signal(barrier, inc=1, device_id={"tracer": target(s)}, device_id_type=MESH)
    pl.semaphore_wait(barrier, 2 + ranks - 1)

    for copy in depth_edges():
        copy.start()

    def start_edges(n, carry):
        for copy in current_edges(n) + species_edges(n):
            copy.start()
        return carry

    lax.fori_loop(0, chunks, start_edges, 0)
    for copy in heat_edges():
        copy.start()

    tot[...] = jnp.zeros_like(tot)
    dep_local.wait()
    fc_local.wait()
    for copy in depth_edges():
        copy.wait()
    lane = lane_index((full, width))

    def advance(n):
        species_local(n).wait()
        for copy in current_edges(n) + species_edges(n):
            copy.wait_recv()
        block = target(n // nc)
        level_0 = first_level(n)

        def one_level(i, carry):
            lev = level_0 + i
            wet = jnp.where(lev < dext[...], 1.0, 0.0)
            es = sub_step * (fext[0, lev] * wet * east(wet))
            ns = sub_step * (fext[1, lev] * wet * north(wet))

            def one_tracer(t, acc):
                c = substep(ext[t, lev], es, ns, lane)
                c = substep(c, es, ns, lane)[PAD:PAD + rows]
                adv[t, lev] = c
                return acc + att[r * nt + t] * jnp.abs(c)

            tot[block] = lax.fori_loop(0, nt, one_tracer, tot[block])
            return carry

        lax.fori_loop(0, q, one_level, 0)

    def advance_send(n, carry):
        advance(n)
        block_copy(n).start()
        return carry

    def advance_keep(n, carry):
        advance(n)
        own_copy(n).start()
        return carry

    lax.fori_loop(0, chunks - nc, advance_send, 0)
    lax.fori_loop(chunks - nc, chunks, advance_keep, 0)

    above = jnp.zeros((rows, width), jnp.float32)
    for place in range(ranks):
        pre[place] = above
        above = above + tot[place]
    own_over = pltpu.make_async_copy(pre.at[r], over.at[r], lf_sem.at[3])
    for s in range(ranks - 1):
        over_copy(s, r).start()
    own_over.start()

    th_local.wait()
    for copy in heat_edges():
        copy.wait()
    coriolis = coriolis_base + beta_plane * lane.astype(jnp.float32) / width

    def momentum(i, carry):
        lev = r * per + i
        u, v, heat_ext = fext[0, lev], fext[1, lev], hext[i]
        wet = jnp.where(lev < dext[...], 1.0, 0.0)
        v_east, u_west = east(v), west(u)
        v_bar = 0.25 * (v + v_east + south(v) + south(v_east))
        u_bar = 0.25 * (u + u_west + north(u) + north(u_west))
        new_u = u + step_duration * (
            coriolis * v_bar - gravity * (east(heat_ext) - heat_ext) + viscosity * laplacian(u)
        )
        new_v = v + step_duration * (
            -coriolis * u_bar - gravity * (north(heat_ext) - heat_ext) + viscosity * laplacian(v)
        )
        vel[0, i] = (wet * east(wet) * new_u)[PAD:PAD + rows]
        vel[1, i] = (wet * north(wet) * new_v)[PAD:PAD + rows]
        warmer = heat_ext + step_duration * spreading_coefficient * laplacian(heat_ext)
        heat[i] = warmer[PAD:PAD + rows]
        return carry

    lax.fori_loop(0, per, momentum, 0)

    def drain_edges(n, carry):
        for copy in current_edges(n) + species_edges(n):
            copy.wait_send()
        return carry

    lax.fori_loop(0, chunks, drain_edges, 0)

    def drain_own(n, carry):
        own_copy(n).wait()
        return carry

    lax.fori_loop(chunks - nc, chunks, drain_own, 0)
    own_over.wait()

    def drain_blocks(n, carry):
        block_arrival(n).wait_recv()
        block_copy(n).wait_send()
        return carry

    lax.fori_loop(0, chunks - nc, drain_blocks, 0)
    for s in range(ranks - 1):
        over_copy(s, source(s)).wait_recv()
        over_copy(s, r).wait_send()


def react_kernel(
    levels, per,
    cells, over, vel, heat, dep, sun, eaten, att, rate,
    out, vel_out, temp_out,
    sat, depth_tau, eater,
):
    step = pl.program_id(0)
    r = lax.axis_index("tracer")
    count = cells.shape[0]
    scale = column_optical / levels

    @pl.when(step == 0)
    def _():
        above = over[0]
        for place in range(1, over.shape[0]):
            above = above + over[place]
        clear = (r * per).astype(jnp.float32) * water_clear
        depth_tau[...] = (above + clear) * scale
        for t in range(count):
            eater[eaten[t]] = t

    vel_out[...] = vel[...]
    total = jnp.full(dep.shape, water_clear, jnp.float32)
    for t in range(count):
        x = cells[t, 0]
        size = jnp.abs(x)
        total = total + att[t] * size
        sat[t] = x / (nutrient_half + size)
    optical = total * scale
    tau = depth_tau[...]
    depth_tau[...] = tau + optical
    wet = jnp.where(r * per + step < dep[...], 1.0, 0.0)
    caught = sun[...] * jnp.exp(-tau) * (1.0 - jnp.exp(-optical))
    mean_light = caught / optical
    gain = wet * (mean_light / (mean_light + light_half))
    temp_out[0] = wet * (heat[0] + warming_coefficient * (caught * wet))
    for t in range(count):
        food, by = eaten[t], eater[t]
        x = cells[t, 0]
        change = rate[t] * (x * sat[food]) - rate[by] * (cells[by, 0] * sat[t])
        out[t, 0] = x + gain * change


def solution(mesh):
    tiles, ranks = mesh.shape["tile"], mesh.shape["tracer"]
    cores = 2 if ranks % 2 == 0 else 1

    def on_device(
        species_amounts,
        face_currents,
        thermal_anomaly,
        layer_total_per_profile,
        consumed_species,
        attenuation_factor,
        intake_speedup,
        incoming_sunshine,
    ):
        nt, nl, rows, width = species_amounts.shape
        per = nl // ranks
        q = 2 if per % 2 == 0 else 1
        chunks = nl // q
        full = rows + 2 * PAD
        f32 = jnp.float32
        any_space = pl.BlockSpec(memory_space=pl.ANY)
        vmem = pl.BlockSpec(memory_space=pltpu.VMEM)
        smem = pl.BlockSpec(memory_space=pltpu.SMEM)
        dma = pltpu.SemaphoreType.DMA
        cells, over, vel, heat = pl.pallas_call(
            functools.partial(transport_kernel, tiles, ranks, cores, q),
            out_shape=(
                jax.ShapeDtypeStruct((ranks * nt, per, rows, width), f32),
                jax.ShapeDtypeStruct((ranks, rows, width), f32),
                jax.ShapeDtypeStruct((2, per, rows, width), f32),
                jax.ShapeDtypeStruct((per, rows, width), f32),
            ),
            in_specs=[any_space] * 4 + [smem],
            out_specs=(any_space, any_space, vmem, vmem),
            scratch_shapes=[
                pltpu.VMEM((nt, nl, full, width), f32),
                pltpu.VMEM((2, nl, full, width), f32),
                pltpu.VMEM((per, full, width), f32),
                pltpu.VMEM((full, width), jnp.int32),
                pltpu.VMEM((nt, nl, rows, width), f32),
                pltpu.VMEM((ranks, rows, width), f32),
                pltpu.VMEM((ranks, rows, width), f32),
                dma((chunks, 2)), dma((chunks, 2)),
                dma((chunks, 2)), dma((chunks, 2)),
                dma((2, 2)), dma((2, 2)),
                dma((chunks,)), dma((chunks,)),
                dma((ranks,)), dma((ranks,)),
                dma((chunks,)), dma((4,)), dma((1,)), dma((per // q,)),
            ],
            compiler_params=pltpu.CompilerParams(
                collective_id=0, has_side_effects=True, vmem_limit_bytes=32 * 2**20
            ),
            name="transport",
        )(
            species_amounts, face_currents, thermal_anomaly,
            layer_total_per_profile, attenuation_factor,
        )
        count = ranks * nt
        column = pl.BlockSpec((count, 1, rows, width), lambda i: (0, i, 0, 0))
        flow = pl.BlockSpec((2, 1, rows, width), lambda i: (0, i, 0, 0))
        sheet = pl.BlockSpec((1, rows, width), lambda i: (i, 0, 0))
        flat = pl.BlockSpec((rows, width), lambda i: (0, 0))
        return pl.pallas_call(
            functools.partial(react_kernel, nl, per),
            grid=(per,),
            out_shape=(
                jax.ShapeDtypeStruct((count, per, rows, width), f32),
                jax.ShapeDtypeStruct((2, per, rows, width), f32),
                jax.ShapeDtypeStruct((per, rows, width), f32),
            ),
            in_specs=[
                column,
                pl.BlockSpec((ranks, rows, width), lambda i: (0, 0, 0)),
                flow, sheet, flat, flat, smem, smem, smem,
            ],
            out_specs=(column, flow, sheet),
            scratch_shapes=[
                pltpu.VMEM((count, rows, width), f32),
                pltpu.VMEM((rows, width), f32),
                pltpu.SMEM((count,), jnp.int32),
            ],
            compiler_params=pltpu.CompilerParams(
                dimension_semantics=("arbitrary",), vmem_limit_bytes=16 * 2**20
            ),
            name="react",
        )(
            cells, over, vel, heat, layer_total_per_profile, incoming_sunshine,
            consumed_species, attenuation_factor, intake_speedup,
        )

    return jax.shard_map(
        on_device,
        mesh=mesh,
        in_specs=(
            P(("groups", "tracer"), None, "tile", None),
            P(None, "groups", "tile", None),
            P(("groups", "tracer"), "tile", None),
            P(("groups", "tile"), None),
            P(),
            P(),
            P(),
            P(("groups", "tile"), None),
        ),
        out_specs=(
            P("groups", "tracer", "tile", None),
            P(None, ("groups", "tracer"), "tile", None),
            P(("groups", "tracer"), "tile", None),
        ),
        check_vma=False,
    )
```

```python
import functools

import jax
import jax.numpy as jnp
from jax import lax
from jax.experimental import pallas as pl
from jax.experimental.pallas import tpu as pltpu
from jax.sharding import PartitionSpec as P

MESH = pl.DeviceIdType.MESH

sub_step = 0.45
step_duration = 0.2
gravity = 0.5
viscosity = 0.2
coriolis_base = 0.5
beta_plane = 0.5
spreading_coefficient = 0.2
water_clear = 0.05
column_optical = 3.0
warming_coefficient = 5.0
light_half = 0.3
nutrient_half = 0.5

PAD = 8
EDGE = 4


def lane_index(shape):
    return lax.broadcasted_iota(jnp.int32, shape, len(shape) - 1)


def east(x):
    return pltpu.roll(x, x.shape[0] - 1, 0)


def west(x):
    return pltpu.roll(x, 1, 0)


def north(x):
    return jnp.where(lane_index(x.shape) == x.shape[1] - 1, 0.0, pltpu.roll(x, x.shape[1] - 1, 1))


def south(x):
    return jnp.where(lane_index(x.shape) == 0, 0.0, pltpu.roll(x, 1, 1))


def minmod(a, b):
    return jnp.maximum(jnp.minimum(a, b), 0.0) + jnp.minimum(jnp.maximum(a, b), 0.0)


def laplacian(x):
    return east(x) + west(x) + north(x) + south(x) - 4.0 * x


def substep(c, es, ns, lane):
    last = c.shape[1] - 1
    d = east(c) - c
    half = 0.5 * minmod(west(d), d)
    flux = es * jnp.where(es > 0.0, c + half, east(c - half))
    spread = flux - west(flux)
    d = jnp.where(lane == last, 0.0, pltpu.roll(c, last, 1)) - c
    half = 0.5 * minmod(jnp.where(lane == 0, c, pltpu.roll(d, 1, 1)), d)
    flux = ns * jnp.where(ns > 0.0, c + half, pltpu.roll(c - half, last, 1))
    return c - (spread + (flux - pltpu.roll(flux, 1, 1)))


def transport_kernel(
    tiles, ranks, cores, q,
    sp, fc, th, dep, att,
    cells, over, vel, heat,
    ext, fext, hext, dext, adv, tot, pre,
    h_send, h_recv, f_send, f_recv, s_send, s_recv, d_send, d_recv, o_send, o_recv,
    l_sem, lf_sem, ls_sem, own_sem,
):
    nt, nl, rows, width = sp.shape
    per = nl // ranks
    nc = per // q
    chips = ranks // cores
    chunks = ranks * nc
    full = rows + 2 * PAD
    r = lax.axis_index("tracer")
    z = lax.axis_index("tile")
    a, b = r // cores, lax.rem(r, cores)
    up, down = lax.rem(z + 1, tiles), lax.rem(z + tiles - 1, tiles)

    def target(s):
        ka, kb = lax.rem(1 + s // cores, chips), cores - 1 - lax.rem(s, cores)
        return lax.rem(a + ka, chips) * cores + lax.rem(b + kb, cores)

    def source(s):
        ka, kb = lax.rem(1 + s // cores, chips), cores - 1 - lax.rem(s, cores)
        return lax.rem(a + chips - ka, chips) * cores + lax.rem(b + cores - kb, cores)

    def first_level(n):
        return target(n // nc) * per + lax.rem(n, nc) * q

    low_rows = pl.ds(0, EDGE)
    high_rows = pl.ds(rows - EDGE, EDGE)
    from_low = pl.ds(PAD - EDGE, EDGE)
    from_high = pl.ds(PAD + rows, EDGE)
    body = pl.ds(PAD, rows)

    def pair(src, dst, lead, send, recv, at):
        return (
            pltpu.make_async_remote_copy(
                src.at[lead + (high_rows,)], dst.at[lead + (from_low,)],
                send.at[at + (0,)], recv.at[at + (0,)],
                device_id={"tile": up}, device_id_type=MESH,
            ),
            pltpu.make_async_remote_copy(
                src.at[lead + (low_rows,)], dst.at[lead + (from_high,)],
                send.at[at + (1,)], recv.at[at + (1,)],
                device_id={"tile": down}, device_id_type=MESH,
            ),
        )

    def species_edges(n):
        lead = (slice(None), pl.ds(first_level(n), q))
        return pair(sp, ext, lead, h_send, h_recv, (n,))

    def current_edges(n):
        lead = (slice(None), pl.ds(first_level(n), q))
        return pair(fc, fext, lead, f_send, f_recv, (n,))

    def heat_edges():
        return pair(th, hext, (slice(None),), s_send, s_recv, (0,))

    def depth_edges():
        return pair(dep, dext, (), s_send, s_recv, (1,))

    def species_local(n):
        lev = pl.ds(first_level(n), q)
        return pltpu.make_async_copy(sp.at[:, lev], ext.at[:, lev, body], l_sem.at[n])

    def block_copy(n):
        s, c = n // nc, lax.rem(n, nc)
        return pltpu.make_async_remote_copy(
            adv.at[:, pl.ds(first_level(n), q)],
            cells.at[pl.ds(r * nt, nt), pl.ds(c * q, q)],
            d_send.at[n], d_recv.at[n],
            device_id={"tracer": target(s)}, device_id_type=MESH,
        )

    def block_arrival(n):
        s, c = n // nc, lax.rem(n, nc)
        return pltpu.make_async_remote_copy(
            adv.at[:, pl.ds(first_level(n), q)],
            cells.at[pl.ds(source(s) * nt, nt), pl.ds(c * q, q)],
            d_send.at[n], d_recv.at[n],
            device_id={"tracer": target(s)}, device_id_type=MESH,
        )

    def own_copy(n):
        c = lax.rem(n, nc)
        return pltpu.make_async_copy(
            adv.at[:, pl.ds(first_level(n), q)],
            cells.at[pl.ds(r * nt, nt), pl.ds(c * q, q)],
            own_sem.at[c],
        )

    def over_copy(s, place):
        return pltpu.make_async_remote_copy(
            pre.at[target(s)], over.at[place], o_send.at[s], o_recv.at[s],
            device_id={"tracer": target(s)}, device_id_type=MESH,
        )

    fc_local = pltpu.make_async_copy(fc, fext.at[:, :, body], lf_sem.at[0])
    dep_local = pltpu.make_async_copy(dep, dext.at[body], lf_sem.at[1])
    th_local = pltpu.make_async_copy(th, hext.at[:, body], lf_sem.at[2])
    dep_local.start()
    fc_local.start()

    def start_local(n, carry):
        species_local(n).start()
        return carry

    lax.fori_loop(0, chunks, start_local, 0)
    th_local.start()

    barrier = pltpu.get_barrier_semaphore()
    for place in (up, down):
        pl.semaphore_signal(barrier, inc=1, device_id={"tile": place}, device_id_type=MESH)
    for s in range(ranks - 1):
        pl.semaphore_signal(barrier, inc=1, device_id={"tracer": target(s)}, device_id_type=MESH)
    pl.semaphore_wait(barrier, 2 + ranks - 1)

    for copy in depth_edges():
        copy.start()

    def start_edges(n, carry):
        for copy in current_edges(n) + species_edges(n):
            copy.start()
        return carry

    lax.fori_loop(0, chunks, start_edges, 0)
    for copy in heat_edges():
        copy.start()

    tot[...] = jnp.zeros_like(tot)
    dep_local.wait()
    fc_local.wait()
    for copy in depth_edges():
        copy.wait()
    lane = lane_index((full, width))

    def advance(n):
        species_local(n).wait()
        for copy in current_edges(n) + species_edges(n):
            copy.wait_recv()
        block = target(n // nc)
        level_0 = first_level(n)

        def one_level(i, carry):
            lev = level_0 + i
            wet = jnp.where(lev < dext[...], 1.0, 0.0)
            es = sub_step * (fext[0, lev] * wet * east(wet))
            ns = sub_step * (fext[1, lev] * wet * north(wet))

            def one_tracer(t, acc):
                c = substep(ext[t, lev], es, ns, lane)
                c = substep(c, es, ns, lane)[PAD:PAD + rows]
                adv[t, lev] = c
                return acc + att[r * nt + t] * jnp.abs(c)

            tot[block] = lax.fori_loop(0, nt, one_tracer, tot[block], unroll=4)
            return carry

        lax.fori_loop(0, q, one_level, 0)

    def advance_send(n, carry):
        advance(n)
        block_copy(n).start()
        return carry

    def advance_keep(n, carry):
        advance(n)
        own_copy(n).start()
        return carry

    lax.fori_loop(0, chunks - nc, advance_send, 0)
    lax.fori_loop(chunks - nc, chunks, advance_keep, 0)

    above = jnp.zeros((rows, width), jnp.float32)
    for place in range(ranks):
        pre[place] = above
        above = above + tot[place]
    own_over = pltpu.make_async_copy(pre.at[r], over.at[r], lf_sem.at[3])
    for s in range(ranks - 1):
        over_copy(s, r).start()
    own_over.start()

    th_local.wait()
    for copy in heat_edges():
        copy.wait()
    coriolis = coriolis_base + beta_plane * lane.astype(jnp.float32) / width

    def momentum(i, carry):
        lev = r * per + i
        u, v, heat_ext = fext[0, lev], fext[1, lev], hext[i]
        wet = jnp.where(lev < dext[...], 1.0, 0.0)
        v_east, u_west = east(v), west(u)
        v_bar = 0.25 * (v + v_east + south(v) + south(v_east))
        u_bar = 0.25 * (u + u_west + north(u) + north(u_west))
        new_u = u + step_duration * (
            coriolis * v_bar - gravity * (east(heat_ext) - heat_ext) + viscosity * laplacian(u)
        )
        new_v = v + step_duration * (
            -coriolis * u_bar - gravity * (north(heat_ext) - heat_ext) + viscosity * laplacian(v)
        )
        vel[0, i] = (wet * east(wet) * new_u)[PAD:PAD + rows]
        vel[1, i] = (wet * north(wet) * new_v)[PAD:PAD + rows]
        warmer = heat_ext + step_duration * spreading_coefficient * laplacian(heat_ext)
        heat[i] = warmer[PAD:PAD + rows]
        return carry

    lax.fori_loop(0, per, momentum, 0)

    def drain_edges(n, carry):
        for copy in current_edges(n) + species_edges(n):
            copy.wait_send()
        return carry

    lax.fori_loop(0, chunks, drain_edges, 0)

    def drain_own(n, carry):
        own_copy(n).wait()
        return carry

    lax.fori_loop(chunks - nc, chunks, drain_own, 0)
    own_over.wait()

    def drain_blocks(n, carry):
        block_arrival(n).wait_recv()
        block_copy(n).wait_send()
        return carry

    lax.fori_loop(0, chunks - nc, drain_blocks, 0)
    for s in range(ranks - 1):
        over_copy(s, source(s)).wait_recv()
        over_copy(s, r).wait_send()


def react_kernel(
    levels, per,
    cells, over, vel, heat, dep, sun, eaten, att, rate,
    out, vel_out, temp_out,
    sat, depth_tau, eater,
):
    step = pl.program_id(0)
    r = lax.axis_index("tracer")
    count = cells.shape[0]
    scale = column_optical / levels

    @pl.when(step == 0)
    def _():
        above = over[0]
        for place in range(1, over.shape[0]):
            above = above + over[place]
        clear = (r * per).astype(jnp.float32) * water_clear
        depth_tau[...] = (above + clear) * scale
        for t in range(count):
            eater[eaten[t]] = t

    vel_out[...] = vel[...]
    total = jnp.full(dep.shape, water_clear, jnp.float32)
    for t in range(count):
        x = cells[t, 0]
        size = jnp.abs(x)
        total = total + att[t] * size
        sat[t] = x / (nutrient_half + size)
    optical = total * scale
    tau = depth_tau[...]
    depth_tau[...] = tau + optical
    wet = jnp.where(r * per + step < dep[...], 1.0, 0.0)
    caught = sun[...] * jnp.exp(-tau) * (1.0 - jnp.exp(-optical))
    mean_light = caught / optical
    gain = wet * (mean_light / (mean_light + light_half))
    temp_out[0] = wet * (heat[0] + warming_coefficient * (caught * wet))
    for t in range(count):
        food, by = eaten[t], eater[t]
        x = cells[t, 0]
        change = rate[t] * (x * sat[food]) - rate[by] * (cells[by, 0] * sat[t])
        out[t, 0] = x + gain * change


def solution(mesh):
    tiles, ranks = mesh.shape["tile"], mesh.shape["tracer"]
    cores = 2 if ranks % 2 == 0 else 1

    def on_device(
        species_amounts,
        face_currents,
        thermal_anomaly,
        layer_total_per_profile,
        consumed_species,
        attenuation_factor,
        intake_speedup,
        incoming_sunshine,
    ):
        nt, nl, rows, width = species_amounts.shape
        per = nl // ranks
        q = 2 if per % 2 == 0 else 1
        chunks = nl // q
        full = rows + 2 * PAD
        f32 = jnp.float32
        any_space = pl.BlockSpec(memory_space=pl.ANY)
        vmem = pl.BlockSpec(memory_space=pltpu.VMEM)
        smem = pl.BlockSpec(memory_space=pltpu.SMEM)
        dma = pltpu.SemaphoreType.DMA
        cells, over, vel, heat = pl.pallas_call(
            functools.partial(transport_kernel, tiles, ranks, cores, q),
            out_shape=(
                jax.ShapeDtypeStruct((ranks * nt, per, rows, width), f32),
                jax.ShapeDtypeStruct((ranks, rows, width), f32),
                jax.ShapeDtypeStruct((2, per, rows, width), f32),
                jax.ShapeDtypeStruct((per, rows, width), f32),
            ),
            in_specs=[any_space] * 4 + [smem],
            out_specs=(any_space, any_space, vmem, vmem),
            scratch_shapes=[
                pltpu.VMEM((nt, nl, full, width), f32),
                pltpu.VMEM((2, nl, full, width), f32),
                pltpu.VMEM((per, full, width), f32),
                pltpu.VMEM((full, width), jnp.int32),
                pltpu.VMEM((nt, nl, rows, width), f32),
                pltpu.VMEM((ranks, rows, width), f32),
                pltpu.VMEM((ranks, rows, width), f32),
                dma((chunks, 2)), dma((chunks, 2)),
                dma((chunks, 2)), dma((chunks, 2)),
                dma((2, 2)), dma((2, 2)),
                dma((chunks,)), dma((chunks,)),
                dma((ranks,)), dma((ranks,)),
                dma((chunks,)), dma((4,)), dma((1,)), dma((per // q,)),
            ],
            compiler_params=pltpu.CompilerParams(
                collective_id=0, has_side_effects=True
            ),
            name="transport",
        )(
            species_amounts, face_currents, thermal_anomaly,
            layer_total_per_profile, attenuation_factor,
        )
        count = ranks * nt
        column = pl.BlockSpec((count, 1, rows, width), lambda i: (0, i, 0, 0))
        flow = pl.BlockSpec((2, 1, rows, width), lambda i: (0, i, 0, 0))
        sheet = pl.BlockSpec((1, rows, width), lambda i: (i, 0, 0))
        flat = pl.BlockSpec((rows, width), lambda i: (0, 0))
        return pl.pallas_call(
            functools.partial(react_kernel, nl, per),
            grid=(per,),
            out_shape=(
                jax.ShapeDtypeStruct((count, per, rows, width), f32),
                jax.ShapeDtypeStruct((2, per, rows, width), f32),
                jax.ShapeDtypeStruct((per, rows, width), f32),
            ),
            in_specs=[
                column,
                pl.BlockSpec((ranks, rows, width), lambda i: (0, 0, 0)),
                flow, sheet, flat, flat, smem, smem, smem,
            ],
            out_specs=(column, flow, sheet),
            scratch_shapes=[
                pltpu.VMEM((count, rows, width), f32),
                pltpu.VMEM((rows, width), f32),
                pltpu.SMEM((count,), jnp.int32),
            ],
            compiler_params=pltpu.CompilerParams(
                dimension_semantics=("arbitrary",)
            ),
            name="react",
        )(
            cells, over, vel, heat, layer_total_per_profile, incoming_sunshine,
            consumed_species, attenuation_factor, intake_speedup,
        )

    return jax.shard_map(
        on_device,
        mesh=mesh,
        in_specs=(
            P(("groups", "tracer"), None, "tile", None),
            P(None, "groups", "tile", None),
            P(("groups", "tracer"), "tile", None),
            P(("groups", "tile"), None),
            P(),
            P(),
            P(),
            P(("groups", "tile"), None),
        ),
        out_specs=(
            P("groups", "tracer", "tile", None),
            P(None, ("groups", "tracer"), "tile", None),
            P(("groups", "tracer"), "tile", None),
        ),
        check_vma=False,
    )
```

```python
import functools

import jax
import jax.numpy as jnp
from jax import lax
from jax.experimental import pallas as pl
from jax.experimental.pallas import tpu as pltpu
from jax.sharding import PartitionSpec as P

MESH = pl.DeviceIdType.MESH

sub_step = 0.45
step_duration = 0.2
gravity = 0.5
viscosity = 0.2
coriolis_base = 0.5
beta_plane = 0.5
spreading_coefficient = 0.2
water_clear = 0.05
column_optical = 3.0
warming_coefficient = 5.0
light_half = 0.3
nutrient_half = 0.5

PAD = 8
EDGE = 4


def lane_index(shape):
    return lax.broadcasted_iota(jnp.int32, shape, len(shape) - 1)


def east(x):
    return pltpu.roll(x, x.shape[0] - 1, 0)


def west(x):
    return pltpu.roll(x, 1, 0)


def north(x):
    return jnp.where(lane_index(x.shape) == x.shape[1] - 1, 0.0, pltpu.roll(x, x.shape[1] - 1, 1))


def south(x):
    return jnp.where(lane_index(x.shape) == 0, 0.0, pltpu.roll(x, 1, 1))


def minmod(a, b):
    return jnp.maximum(jnp.minimum(a, b), 0.0) + jnp.minimum(jnp.maximum(a, b), 0.0)


def laplacian(x):
    return east(x) + west(x) + north(x) + south(x) - 4.0 * x


def substep(c, es, ns, lane):
    last = c.shape[1] - 1
    d = east(c) - c
    half = 0.5 * minmod(west(d), d)
    flux = es * jnp.where(es > 0.0, c + half, east(c - half))
    spread = flux - west(flux)
    d = jnp.where(lane == last, 0.0, pltpu.roll(c, last, 1)) - c
    half = 0.5 * minmod(jnp.where(lane == 0, c, pltpu.roll(d, 1, 1)), d)
    flux = ns * jnp.where(ns > 0.0, c + half, pltpu.roll(c - half, last, 1))
    return c - (spread + (flux - pltpu.roll(flux, 1, 1)))


def transport_kernel(
    tiles, ranks, cores, q,
    sp, fc, th, dep, att,
    cells, over, vel, heat,
    ext, fext, hext, dext, adv, tot, pre,
    h_send, h_recv, f_send, f_recv, s_send, s_recv, d_send, d_recv, o_send, o_recv,
    l_sem, lf_sem, ls_sem, own_sem,
):
    nt, nl, rows, width = sp.shape
    per = nl // ranks
    nc = per // q
    chips = ranks // cores
    chunks = ranks * nc
    full = rows + 2 * PAD
    r = lax.axis_index("tracer")
    z = lax.axis_index("tile")
    a, b = r // cores, lax.rem(r, cores)
    up, down = lax.rem(z + 1, tiles), lax.rem(z + tiles - 1, tiles)

    def target(s):
        ka, kb = lax.rem(1 + s // cores, chips), cores - 1 - lax.rem(s, cores)
        return lax.rem(a + ka, chips) * cores + lax.rem(b + kb, cores)

    def source(s):
        ka, kb = lax.rem(1 + s // cores, chips), cores - 1 - lax.rem(s, cores)
        return lax.rem(a + chips - ka, chips) * cores + lax.rem(b + cores - kb, cores)

    def first_level(n):
        return target(n // nc) * per + lax.rem(n, nc) * q

    low_rows = pl.ds(0, EDGE)
    high_rows = pl.ds(rows - EDGE, EDGE)
    from_low = pl.ds(PAD - EDGE, EDGE)
    from_high = pl.ds(PAD + rows, EDGE)
    body = pl.ds(PAD, rows)

    def pair(src, dst, lead, send, recv, at):
        return (
            pltpu.make_async_remote_copy(
                src.at[lead + (high_rows,)], dst.at[lead + (from_low,)],
                send.at[at + (0,)], recv.at[at + (0,)],
                device_id={"tile": up}, device_id_type=MESH,
            ),
            pltpu.make_async_remote_copy(
                src.at[lead + (low_rows,)], dst.at[lead + (from_high,)],
                send.at[at + (1,)], recv.at[at + (1,)],
                device_id={"tile": down}, device_id_type=MESH,
            ),
        )

    def species_edges(n):
        lead = (slice(None), pl.ds(first_level(n), q))
        return pair(sp, ext, lead, h_send, h_recv, (n,))

    def current_edges(n):
        lead = (slice(None), pl.ds(first_level(n), q))
        return pair(fc, fext, lead, f_send, f_recv, (n,))

    def heat_edges():
        return pair(th, hext, (slice(None),), s_send, s_recv, (0,))

    def depth_edges():
        return pair(dep, dext, (), s_send, s_recv, (1,))

    def species_local(n):
        lev = pl.ds(first_level(n), q)
        return pltpu.make_async_copy(sp.at[:, lev], ext.at[:, lev, body], l_sem.at[n])

    def block_copy(n):
        s, c = n // nc, lax.rem(n, nc)
        return pltpu.make_async_remote_copy(
            adv.at[:, pl.ds(first_level(n), q)],
            cells.at[pl.ds(r * nt, nt), pl.ds(c * q, q)],
            d_send.at[n], d_recv.at[n],
            device_id={"tracer": target(s)}, device_id_type=MESH,
        )

    def block_arrival(n):
        s, c = n // nc, lax.rem(n, nc)
        return pltpu.make_async_remote_copy(
            adv.at[:, pl.ds(first_level(n), q)],
            cells.at[pl.ds(source(s) * nt, nt), pl.ds(c * q, q)],
            d_send.at[n], d_recv.at[n],
            device_id={"tracer": target(s)}, device_id_type=MESH,
        )

    def own_copy(n):
        c = lax.rem(n, nc)
        return pltpu.make_async_copy(
            adv.at[:, pl.ds(first_level(n), q)],
            cells.at[pl.ds(r * nt, nt), pl.ds(c * q, q)],
            own_sem.at[c],
        )

    def over_copy(s, place):
        return pltpu.make_async_remote_copy(
            pre.at[target(s)], over.at[place], o_send.at[s], o_recv.at[s],
            device_id={"tracer": target(s)}, device_id_type=MESH,
        )

    fc_local = pltpu.make_async_copy(fc, fext.at[:, :, body], lf_sem.at[0])
    dep_local = pltpu.make_async_copy(dep, dext.at[body], lf_sem.at[1])
    th_local = pltpu.make_async_copy(th, hext.at[:, body], lf_sem.at[2])
    dep_local.start()
    fc_local.start()

    def start_local(n, carry):
        species_local(n).start()
        return carry

    lax.fori_loop(0, chunks, start_local, 0)
    th_local.start()

    barrier = pltpu.get_barrier_semaphore()
    for place in (up, down):
        pl.semaphore_signal(barrier, inc=1, device_id={"tile": place}, device_id_type=MESH)
    for s in range(ranks - 1):
        pl.semaphore_signal(barrier, inc=1, device_id={"tracer": target(s)}, device_id_type=MESH)
    pl.semaphore_wait(barrier, 2 + ranks - 1)

    for copy in depth_edges():
        copy.start()

    def start_edges(n, carry):
        for copy in current_edges(n) + species_edges(n):
            copy.start()
        return carry

    lax.fori_loop(0, chunks, start_edges, 0)
    for copy in heat_edges():
        copy.start()

    tot[...] = jnp.zeros_like(tot)
    dep_local.wait()
    fc_local.wait()
    for copy in depth_edges():
        copy.wait()
    lane = lane_index((full, width))

    def advance(n):
        species_local(n).wait()
        for copy in current_edges(n) + species_edges(n):
            copy.wait_recv()
        block = target(n // nc)
        level_0 = first_level(n)

        def one_level(i, carry):
            lev = level_0 + i
            wet = jnp.where(lev < dext[...], 1.0, 0.0)
            es = sub_step * (fext[0, lev] * wet * east(wet))
            ns = sub_step * (fext[1, lev] * wet * north(wet))

            def one_tracer(t, acc):
                c = substep(ext[t, lev], es, ns, lane)
                c = substep(c, es, ns, lane)[PAD:PAD + rows]
                adv[t, lev] = c
                return acc + att[r * nt + t] * jnp.abs(c)

            tot[block] = lax.fori_loop(0, nt, one_tracer, tot[block], unroll=True)
            return carry

        lax.fori_loop(0, q, one_level, 0)

    def advance_send(n, carry):
        advance(n)
        block_copy(n).start()
        return carry

    def advance_keep(n, carry):
        advance(n)
        own_copy(n).start()
        return carry

    lax.fori_loop(0, chunks - nc, advance_send, 0)
    lax.fori_loop(chunks - nc, chunks, advance_keep, 0)

    above = jnp.zeros((rows, width), jnp.float32)
    for place in range(ranks):
        pre[place] = above
        above = above + tot[place]
    own_over = pltpu.make_async_copy(pre.at[r], over.at[r], lf_sem.at[3])
    for s in range(ranks - 1):
        over_copy(s, r).start()
    own_over.start()

    th_local.wait()
    for copy in heat_edges():
        copy.wait()
    coriolis = coriolis_base + beta_plane * lane.astype(jnp.float32) / width

    def momentum(i, carry):
        lev = r * per + i
        u, v, heat_ext = fext[0, lev], fext[1, lev], hext[i]
        wet = jnp.where(lev < dext[...], 1.0, 0.0)
        v_east, u_west = east(v), west(u)
        v_bar = 0.25 * (v + v_east + south(v) + south(v_east))
        u_bar = 0.25 * (u + u_west + north(u) + north(u_west))
        new_u = u + step_duration * (
            coriolis * v_bar - gravity * (east(heat_ext) - heat_ext) + viscosity * laplacian(u)
        )
        new_v = v + step_duration * (
            -coriolis * u_bar - gravity * (north(heat_ext) - heat_ext) + viscosity * laplacian(v)
        )
        vel[0, i] = (wet * east(wet) * new_u)[PAD:PAD + rows]
        vel[1, i] = (wet * north(wet) * new_v)[PAD:PAD + rows]
        warmer = heat_ext + step_duration * spreading_coefficient * laplacian(heat_ext)
        heat[i] = warmer[PAD:PAD + rows]
        return carry

    lax.fori_loop(0, per, momentum, 0)

    def drain_edges(n, carry):
        for copy in current_edges(n) + species_edges(n):
            copy.wait_send()
        return carry

    lax.fori_loop(0, chunks, drain_edges, 0)

    def drain_own(n, carry):
        own_copy(n).wait()
        return carry

    lax.fori_loop(chunks - nc, chunks, drain_own, 0)
    own_over.wait()

    def drain_blocks(n, carry):
        block_arrival(n).wait_recv()
        block_copy(n).wait_send()
        return carry

    lax.fori_loop(0, chunks - nc, drain_blocks, 0)
    for s in range(ranks - 1):
        over_copy(s, source(s)).wait_recv()
        over_copy(s, r).wait_send()


def react_kernel(
    levels, per,
    cells, over, vel, heat, dep, sun, eaten, att, rate,
    out, vel_out, temp_out,
    sat, depth_tau, eater,
):
    step = pl.program_id(0)
    r = lax.axis_index("tracer")
    count = cells.shape[0]
    scale = column_optical / levels

    @pl.when(step == 0)
    def _():
        above = over[0]
        for place in range(1, over.shape[0]):
            above = above + over[place]
        clear = (r * per).astype(jnp.float32) * water_clear
        depth_tau[...] = (above + clear) * scale
        for t in range(count):
            eater[eaten[t]] = t

    vel_out[...] = vel[...]
    total = jnp.full(dep.shape, water_clear, jnp.float32)
    for t in range(count):
        x = cells[t, 0]
        size = jnp.abs(x)
        total = total + att[t] * size
        sat[t] = x / (nutrient_half + size)
    optical = total * scale
    tau = depth_tau[...]
    depth_tau[...] = tau + optical
    wet = jnp.where(r * per + step < dep[...], 1.0, 0.0)
    caught = sun[...] * jnp.exp(-tau) * (1.0 - jnp.exp(-optical))
    mean_light = caught / optical
    gain = wet * (mean_light / (mean_light + light_half))
    temp_out[0] = wet * (heat[0] + warming_coefficient * (caught * wet))
    for t in range(count):
        food, by = eaten[t], eater[t]
        x = cells[t, 0]
        change = rate[t] * (x * sat[food]) - rate[by] * (cells[by, 0] * sat[t])
        out[t, 0] = x + gain * change


def solution(mesh):
    tiles, ranks = mesh.shape["tile"], mesh.shape["tracer"]
    cores = 2 if ranks % 2 == 0 else 1

    def on_device(
        species_amounts,
        face_currents,
        thermal_anomaly,
        layer_total_per_profile,
        consumed_species,
        attenuation_factor,
        intake_speedup,
        incoming_sunshine,
    ):
        nt, nl, rows, width = species_amounts.shape
        per = nl // ranks
        q = 2 if per % 2 == 0 else 1
        chunks = nl // q
        full = rows + 2 * PAD
        f32 = jnp.float32
        any_space = pl.BlockSpec(memory_space=pl.ANY)
        vmem = pl.BlockSpec(memory_space=pltpu.VMEM)
        smem = pl.BlockSpec(memory_space=pltpu.SMEM)
        dma = pltpu.SemaphoreType.DMA
        cells, over, vel, heat = pl.pallas_call(
            functools.partial(transport_kernel, tiles, ranks, cores, q),
            out_shape=(
                jax.ShapeDtypeStruct((ranks * nt, per, rows, width), f32),
                jax.ShapeDtypeStruct((ranks, rows, width), f32),
                jax.ShapeDtypeStruct((2, per, rows, width), f32),
                jax.ShapeDtypeStruct((per, rows, width), f32),
            ),
            in_specs=[any_space] * 4 + [smem],
            out_specs=(any_space, any_space, vmem, vmem),
            scratch_shapes=[
                pltpu.VMEM((nt, nl, full, width), f32),
                pltpu.VMEM((2, nl, full, width), f32),
                pltpu.VMEM((per, full, width), f32),
                pltpu.VMEM((full, width), jnp.int32),
                pltpu.VMEM((nt, nl, rows, width), f32),
                pltpu.VMEM((ranks, rows, width), f32),
                pltpu.VMEM((ranks, rows, width), f32),
                dma((chunks, 2)), dma((chunks, 2)),
                dma((chunks, 2)), dma((chunks, 2)),
                dma((2, 2)), dma((2, 2)),
                dma((chunks,)), dma((chunks,)),
                dma((ranks,)), dma((ranks,)),
                dma((chunks,)), dma((4,)), dma((1,)), dma((per // q,)),
            ],
            compiler_params=pltpu.CompilerParams(
                collective_id=0, has_side_effects=True
            ),
            name="transport",
        )(
            species_amounts, face_currents, thermal_anomaly,
            layer_total_per_profile, attenuation_factor,
        )
        count = ranks * nt
        column = pl.BlockSpec((count, 1, rows, width), lambda i: (0, i, 0, 0))
        flow = pl.BlockSpec((2, 1, rows, width), lambda i: (0, i, 0, 0))
        sheet = pl.BlockSpec((1, rows, width), lambda i: (i, 0, 0))
        flat = pl.BlockSpec((rows, width), lambda i: (0, 0))
        return pl.pallas_call(
            functools.partial(react_kernel, nl, per),
            grid=(per,),
            out_shape=(
                jax.ShapeDtypeStruct((count, per, rows, width), f32),
                jax.ShapeDtypeStruct((2, per, rows, width), f32),
                jax.ShapeDtypeStruct((per, rows, width), f32),
            ),
            in_specs=[
                column,
                pl.BlockSpec((ranks, rows, width), lambda i: (0, 0, 0)),
                flow, sheet, flat, flat, smem, smem, smem,
            ],
            out_specs=(column, flow, sheet),
            scratch_shapes=[
                pltpu.VMEM((count, rows, width), f32),
                pltpu.VMEM((rows, width), f32),
                pltpu.SMEM((count,), jnp.int32),
            ],
            compiler_params=pltpu.CompilerParams(
                dimension_semantics=("arbitrary",)
            ),
            name="react",
        )(
            cells, over, vel, heat, layer_total_per_profile, incoming_sunshine,
            consumed_species, attenuation_factor, intake_speedup,
        )

    return jax.shard_map(
        on_device,
        mesh=mesh,
        in_specs=(
            P(("groups", "tracer"), None, "tile", None),
            P(None, "groups", "tile", None),
            P(("groups", "tracer"), "tile", None),
            P(("groups", "tile"), None),
            P(),
            P(),
            P(),
            P(("groups", "tile"), None),
        ),
        out_specs=(
            P("groups", "tracer", "tile", None),
            P(None, ("groups", "tracer"), "tile", None),
            P(("groups", "tracer"), "tile", None),
        ),
        check_vma=False,
    )
```
